32 devices in a mesh: paths: 8 (over z, core), stocks: 4 (over y, x).
Axes of the slice: x: 2, y: 2, z: 4, core: 2. Of those that a mesh axis runs over, the one named last changes fastest.
Arguments:
- prices: bfloat16 [256, 131072], P('stocks', 'paths'), may hold values from -18 to 18
- loadings: bfloat16 [256, 32], P('stocks'), may hold values from -0.25 to 0.25
- basis_w: float32 [32, 512], replicated, may hold values from -1 to 1
- basis_bias: float32 [512], replicated, may hold values from -1 to 1
- payoff: bfloat16 [131072], P('paths'), may hold values from -4 to 4
- in_fit: int32 [131072], P('paths'), may hold values 0 or 1
- cotangent: bfloat16 [256, 131072], P('stocks', 'paths'), may hold values from -6 to 6
- shocks: bfloat16 [4, 256, 131072], P(None, 'stocks', 'paths'), may hold values from -6 to 6
- corr_gen: bfloat16 [256, 256], replicated, may hold values from -0.375 to 0.375
- basket: float32 [256], replicated, may hold values from 0.2 to 2
- exercise: int32 [4, 131072], P(None, 'paths'), may hold values 0 or 1
- bucket: int32 [4, 131072], P(None, 'paths'), may hold values from 0 to 255
Outputs:
- delta_out: float32 [256, 131072], P('stocks', 'paths')
- surface: float32 [256, 256], P('stocks', 'paths')
The draws below stay inside these ranges and needn't reach their ends.
All inputs are finite; a program needn't handle non-finite values. No bound on the sum of `in_fit` or of `exercise` on one device may be relied on, other than what follows from the above.
Results may differ from the reference program's by a relative error of at most 0.003.
Values may be sent and summed in bfloat16 or wider, within the bound.
A program may use at most 192 MiB of HBM per device.

```python
import jax
import jax.numpy as jnp
from jax import lax

S = 256
K = 32
B = 512
NK = 256
STEPS = 4
PATHS = 131072


def price_state(key):
    price_key = jax.random.fold_in(key, 101)
    position = jnp.arange(PATHS, dtype=jnp.float32) / PATHS
    random_part = jax.random.truncated_normal(price_key, -6.0, 6.0, (S, PATHS), jnp.float32)
    path_scale = jnp.exp(jnp.log(3.0) * position)
    return (random_part * path_scale[None, :]).astype(jnp.bfloat16)


def loading_table(key):
    load_key = jax.random.fold_in(key, 102)
    limit = min(4.0, 0.25 * S ** 0.5)
    values = jax.random.truncated_normal(load_key, -limit, limit, (S, K), jnp.float32) / S ** 0.5
    values = jnp.clip(values, -0.25, 0.25)
    return values.astype(jnp.bfloat16)


def draw_prices(key, part):
    return price_state(key)


def draw_loadings(key, part):
    return loading_table(key)


def draw_payoff(key, part):
    prices = price_state(key)
    loads = loading_table(key)
    factors = lax.dot_general(loads, prices, (((0,), (0,)), ((), ())), preferred_element_type=jnp.float32)
    directions = jax.random.normal(jax.random.fold_in(key, 103), (2, K), jnp.float32) / K ** 0.5
    levels = jnp.dot(directions, factors, preferred_element_type=jnp.float32, precision=lax.Precision.HIGHEST)
    shaped = 2.0 * jnp.tanh(0.7 * levels[0]) + 0.8 * jnp.abs(jnp.tanh(levels[1])) - 0.4
    noise = 0.3 * jax.random.truncated_normal(jax.random.fold_in(key, 104), -3.0, 3.0, (PATHS,), jnp.float32)
    return jnp.clip(shaped + noise, -4.0, 4.0).astype(jnp.bfloat16)


def with_ends(result, key, low, high):
    longest = result.shape.index(max(result.shape))
    spots = []
    for shift in (0, 1):
        where = [jax.random.randint(jax.random.fold_in(key, axis), (), 0, length) for axis, length in enumerate(result.shape)]
        where[longest] = (where[longest] + shift) % result.shape[longest]
        spots.append(tuple(where))
    return result.at[spots[0]].set(low).at[spots[1]].set(high)


def level_of(own_key, dims, shards, least, top_value):
    level = 1.0
    for axis_at, blocks in shards:
        draws = jax.random.uniform(jax.random.fold_in(jax.random.fold_in(own_key, 6), axis_at), (blocks,), jnp.float32, least / len(shards), top_value / len(shards))
        level = level * jnp.repeat(jnp.exp(draws), dims[axis_at] // blocks).reshape((-1,) + (1,) * (len(dims) - 1 - axis_at))
    return level


def scatter_about(key, dims, scale, bound, shards=(), kind=jnp.bfloat16):
    result = scale * jax.random.normal(key, dims, jnp.float32)
    if shards:
        result = result * level_of(key, dims, shards, -0.22, 0.18)
    return jnp.clip(result, -bound, bound).astype(kind)


def setup_inputs(seed: int = 0) -> dict:
    streams_of = jax.random.split(jax.random.key(seed), 13)
    return {
        "prices": draw_prices(jax.random.fold_in(streams_of[12], 71), 0),
        "loadings": draw_loadings(jax.random.fold_in(streams_of[12], 71), 0),
        "basis_w": scatter_about(streams_of[2], (K, B), K ** -0.5, 1.0, (), jnp.float32),
        "basis_bias": jnp.clip(jax.random.uniform(streams_of[3], (B,), jnp.float32, -1.0, 1.0), -1.0, 1.0),
        "payoff": draw_payoff(jax.random.fold_in(streams_of[12], 71), 0),
        "in_fit": with_ends((jax.random.randint(streams_of[5], (PATHS,), 0, 3) < 2).astype(jnp.int32), jax.random.fold_in(streams_of[5], 1), 0, 1),
        "cotangent": scatter_about(streams_of[6], (S, PATHS), 1.0, 6.0, ((0, 4), (1, 8))),
        "shocks": scatter_about(streams_of[7], (STEPS, S, PATHS), 1.0, 6.0, ((1, 4), (2, 8))),
        "corr_gen": scatter_about(streams_of[8], (S, S), S ** -0.5, 0.375),
        "basket": jnp.clip(jax.random.uniform(streams_of[9], (S,), jnp.float32, 0.2, 2.0), 0.2, 2.0),
        "exercise": with_ends((jax.random.randint(streams_of[10], (STEPS, PATHS), 0, 4) < 1).astype(jnp.int32), jax.random.fold_in(streams_of[10], 1), 0, 1),
        "bucket": with_ends(jax.random.randint(streams_of[11], (STEPS, PATHS), 0, NK), jax.random.fold_in(streams_of[11], 1), 0, NK - 1).astype(jnp.int32),
    }


time_step = 0.25
ridge_weight = 0.1

def make_basis(factors, basis_w, basis_bias):
    raised = jnp.dot(basis_w.T.astype(jnp.float32), factors.astype(jnp.float32), preferred_element_type=jnp.float32, precision=lax.Precision.HIGHEST) + basis_bias[:, None]
    return jnp.tanh(raised).astype(jnp.bfloat16)

def regression_sums(basis, payoff, in_fit):
    picked = basis * in_fit.astype(jnp.bfloat16)[None, :]
    gram_sums = lax.dot_general(picked.astype(jnp.float32), basis.astype(jnp.float32), (((1,), (1,)), ((), ())), preferred_element_type=jnp.float32)
    moment = jnp.dot(picked.astype(jnp.float32), payoff.astype(jnp.float32), preferred_element_type=jnp.float32)
    return (gram_sums, moment)

def solve_coefficients(gram_sums, moment, path_count):
    system = gram_sums / path_count + ridge_weight * jnp.eye(gram_sums.shape[0], dtype=jnp.float32)
    cholesky_factor = jnp.linalg.cholesky(system)
    return jax.scipy.linalg.cho_solve((cholesky_factor, True), moment / path_count)

def reference(prices, loadings, basis_w, basis_bias, payoff, in_fit, cotangent, shocks, corr_gen, basket, exercise, bucket):
    factors = lax.dot_general(loadings.astype(jnp.float32), prices.astype(jnp.float32), (((0,), (0,)), ((), ())), preferred_element_type=jnp.float32)
    basis = make_basis(factors, basis_w, basis_bias)
    gram_sums, moment = regression_sums(basis, payoff, in_fit)
    coefficients = solve_coefficients(gram_sums, moment, PATHS * 1.0)
    continuation = jnp.dot(coefficients.astype(jnp.float32), basis.astype(jnp.float32), preferred_element_type=jnp.float32, precision=lax.Precision.HIGHEST)
    adjoint = cotangent.astype(jnp.float32)
    surface = jnp.zeros((S, NK), jnp.float32)
    strikes = jnp.arange(NK, dtype=jnp.int32)
    for date_index in range(STEPS - 1, -1, -1):
        mixed_rows = jnp.dot(corr_gen.astype(jnp.float32), adjoint.astype(jnp.bfloat16).astype(jnp.float32), preferred_element_type=jnp.float32)
        adjoint = adjoint + time_step * mixed_rows + exercise[date_index].astype(jnp.float32)[None, :] * continuation[None, :] * basket[:, None]
        vega_terms = (adjoint * shocks[date_index].astype(jnp.float32)).astype(jnp.bfloat16)
        one_hot = (bucket[date_index][:, None] == strikes[None, :]).astype(jnp.bfloat16)
        surface = surface + jnp.dot(vega_terms.astype(jnp.float32), one_hot.astype(jnp.float32), preferred_element_type=jnp.float32)
    return (adjoint, surface)
```

```python
import functools

import jax
import jax.numpy as jnp
from jax import lax
from jax.experimental import pallas as pl
from jax.experimental.pallas import tpu as pltpu
from jax.sharding import PartitionSpec as P

NK = 256
STEPS = 4
SUB = 8
BLOCK = 128

time_step = 0.25
ridge_weight = 0.1
HIGHEST = lax.Precision.HIGHEST


def pieces(value):
    high = value.astype(jnp.bfloat16)
    rest = value - high.astype(jnp.float32)
    middle = rest.astype(jnp.bfloat16)
    low = (rest - middle.astype(jnp.float32)).astype(jnp.bfloat16)
    return high, middle, low


def basis_kernel(factors_ref, weights_ref, bias_ref, payoff_ref, fit_ref, basis_ref, sums_ref, packed_ref):
    @pl.when(pl.program_id(0) == 0)
    def _():
        high, middle, low = pieces(weights_ref[...])
        packed_ref[...] = jnp.concatenate([high, high, middle, high, middle, low], axis=1)
        sums_ref[...] = jnp.zeros_like(sums_ref)

    high, middle, low = pieces(factors_ref[...])
    packed_factors = jnp.concatenate([high, middle, high, low, middle, high], axis=0)
    raised = jnp.dot(packed_ref[...], packed_factors, preferred_element_type=jnp.float32)
    basis = jnp.tanh(raised + bias_ref[...]).astype(jnp.bfloat16)
    basis_ref[...] = basis
    fit = fit_ref[...].astype(jnp.bfloat16)
    picked = basis * fit
    contract = (((1,), (1,)), ((), ()))
    functions = basis.shape[0]
    sums_ref[0:functions, :] += lax.dot_general(
        basis, picked, contract, preferred_element_type=jnp.float32
    )
    cash = jnp.broadcast_to(payoff_ref[...], (2 * SUB, basis.shape[1]))
    moment = lax.dot_general(cash, picked, contract, preferred_element_type=jnp.float32)
    sums_ref[functions : functions + SUB, :] += moment[0:SUB]


def basis_and_sums(factors, basis_w, basis_bias, payoff, in_fit):
    rank, functions = basis_w.shape
    paths = factors.shape[1]
    tile = min(1024, paths)
    return pl.pallas_call(
        basis_kernel,
        grid=(paths // tile,),
        in_specs=[
            pl.BlockSpec((rank, tile), lambda i: (0, i)),
            pl.BlockSpec((functions, rank), lambda i: (0, 0)),
            pl.BlockSpec((functions, 1), lambda i: (0, 0)),
            pl.BlockSpec((1, tile), lambda i: (0, i)),
            pl.BlockSpec((1, tile), lambda i: (0, i)),
        ],
        out_specs=[
            pl.BlockSpec((functions, tile), lambda i: (0, i)),
            pl.BlockSpec((functions + SUB, functions), lambda i: (0, 0)),
        ],
        out_shape=[
            jax.ShapeDtypeStruct((functions, paths), jnp.bfloat16),
            jax.ShapeDtypeStruct((functions + SUB, functions), jnp.float32),
        ],
        scratch_shapes=[pltpu.VMEM((functions, 6 * rank), jnp.bfloat16)],
        cost_estimate=pl.CostEstimate(
            flops=2 * functions * paths * (6 * rank + functions),
            bytes_accessed=functions * paths * 2,
            transcendentals=functions * paths,
        ),
        name="basis_sums",
    )(factors, basis_w.T, basis_bias[:, None], payoff[None, :], in_fit[None, :])


def sweep_block(tile_ref):
    size = tile_ref.shape[0]
    rows = lax.broadcasted_iota(jnp.int32, (SUB, size), 0)
    lanes = lax.broadcasted_iota(jnp.int32, (SUB, size), 1)
    all_lanes = lax.broadcasted_iota(jnp.int32, (size, size), 1)
    for start in range(0, size, SUB):
        whole = tile_ref[...]
        columns = [
            jnp.broadcast_to(whole[:, start + c : start + c + 1], (size, size)) for c in range(SUB)
        ]
        pivots = [columns[c][start : start + SUB] for c in range(SUB)]
        strip = whole[start : start + SUB]
        inside = (lanes >= start) & (lanes < start + SUB)
        strip = jnp.where(inside, jnp.where(lanes - start == rows, 1.0, 0.0), strip)
        for j in range(SUB):
            inverse = 1.0 / pivots[j][j : j + 1]
            chosen = strip[j : j + 1] * inverse
            strip = jnp.where(rows == j, chosen, strip - pivots[j] * chosen)
            for c in range(j + 1, SUB):
                moved = pivots[c][j : j + 1] * inverse
                pivots[c] = jnp.where(rows == j, moved, pivots[c] - pivots[j] * moved)
        inside_all = (all_lanes >= start) & (all_lanes < start + SUB)
        updated = jnp.where(inside_all, 0.0, whole)
        for c in range(SUB):
            updated = updated - columns[c] * strip[c : c + 1]
        tile_ref[...] = updated
        tile_ref[start : start + SUB, :] = strip


def solve_kernel(scale, sums_ref, out_ref, system_ref, moment_ref, inverse_ref, reduced_ref, tile_ref):
    size = system_ref.shape[0]
    row_ids = lax.broadcasted_iota(jnp.int32, (size, size), 0)
    lane_ids = lax.broadcasted_iota(jnp.int32, (size, size), 1)
    system_ref[...] = sums_ref[0:size, :] * scale + jnp.where(row_ids == lane_ids, ridge_weight, 0.0)
    moment_ref[...] = sums_ref[size : size + SUB, :] * scale
    strip_lanes = lax.broadcasted_iota(jnp.int32, (BLOCK, size), 1)

    def eliminate(k, carry):
        here = pl.ds(pl.multiple_of(k * BLOCK, BLOCK), BLOCK)
        tile_ref[...] = system_ref[here, here]
        sweep_block(tile_ref)
        inverse = tile_ref[...]
        inverse_ref[here, :] = inverse
        right = jnp.where(strip_lanes >= (k + 1) * BLOCK, system_ref[here, :], 0.0)
        reduced = jnp.dot(inverse, right, preferred_element_type=jnp.float32, precision=HIGHEST)
        reduced_ref[here, :] = reduced
        system_ref[...] -= jnp.dot(
            system_ref[:, here], reduced, preferred_element_type=jnp.float32, precision=HIGHEST
        )
        moment_ref[...] -= jnp.dot(
            moment_ref[:, here], reduced, preferred_element_type=jnp.float32, precision=HIGHEST
        )
        return carry

    blocks = size // BLOCK
    lax.fori_loop(0, blocks, eliminate, 0)
    out_ref[...] = jnp.zeros_like(out_ref)

    def substitute(step, carry):
        k = blocks - 1 - step
        here = pl.ds(pl.multiple_of(k * BLOCK, BLOCK), BLOCK)
        known = lax.dot_general(
            out_ref[...],
            reduced_ref[here, :],
            (((1,), (1,)), ((), ())),
            preferred_element_type=jnp.float32,
            precision=HIGHEST,
        )
        out_ref[:, here] = (
            jnp.dot(
                moment_ref[:, here],
                inverse_ref[here, :],
                preferred_element_type=jnp.float32,
                precision=HIGHEST,
            )
            - known
        )
        return carry

    lax.fori_loop(0, blocks, substitute, 0)


def solve_coefficients(sums, path_count):
    size = sums.shape[1]
    return pl.pallas_call(
        functools.partial(solve_kernel, 1.0 / path_count),
        in_specs=[pl.BlockSpec(memory_space=pltpu.VMEM)],
        out_specs=pl.BlockSpec(memory_space=pltpu.VMEM),
        out_shape=jax.ShapeDtypeStruct((SUB, size), jnp.float32),
        scratch_shapes=[
            pltpu.VMEM((size, size), jnp.float32),
            pltpu.VMEM((SUB, size), jnp.float32),
            pltpu.VMEM((size, BLOCK), jnp.float32),
            pltpu.VMEM((size, size), jnp.float32),
            pltpu.VMEM((BLOCK, BLOCK), jnp.float32),
        ],
        cost_estimate=pl.CostEstimate(
            flops=20_000_000_000, bytes_accessed=sums.size * 4, transcendentals=0
        ),
        name="solve",
    )(sums)


def adjoint_kernel(
    whole_ref, own_ref, shocks_ref, value_ref, exercise_ref, bucket_ref, powers_ref, basket_ref,
    delta_ref, surface_ref, split_ref,
):
    rows = own_ref.shape[0]
    tile = own_ref.shape[1]

    @pl.when(pl.program_id(0) == 0)
    def _():
        high, middle, _ = pieces(powers_ref[...])
        split_ref[0] = high
        split_ref[1] = middle
        surface_ref[...] = jnp.zeros_like(surface_ref)

    whole = whole_ref[...]
    start = own_ref[...].astype(jnp.float32)
    gains = [
        exercise_ref[date : date + 1, :].astype(jnp.float32) * value_ref[...] for date in range(STEPS)
    ]
    strikes = lax.broadcasted_iota(jnp.int32, (NK, tile), 0)
    total = jnp.zeros(surface_ref.shape, jnp.float32)
    for date in range(STEPS - 1, -1, -1):
        power = STEPS - 1 - date
        part = pl.ds(power * rows, rows)
        adjoint = (
            start
            + jnp.dot(split_ref[0, part, :], whole, preferred_element_type=jnp.float32)
            + jnp.dot(split_ref[1, part, :], whole, preferred_element_type=jnp.float32)
        )
        for later in range(date, STEPS):
            adjoint = adjoint + basket_ref[:, later - date : later - date + 1] * gains[later]
        if date == 0:
            delta_ref[...] = adjoint
        vega = (adjoint * shocks_ref[date].astype(jnp.float32)).astype(jnp.bfloat16)
        one_hot = jnp.where(bucket_ref[date : date + 1, :] == strikes, 1.0, 0.0).astype(jnp.bfloat16)
        total = total + lax.dot_general(
            vega, one_hot, (((1,), (1,)), ((), ())), preferred_element_type=jnp.float32
        )
    surface_ref[...] += total


def adjoint_and_surface(whole, own, shocks, value, exercise, bucket, powers, baskets):
    stocks, paths = whole.shape
    rows = own.shape[0]
    tile = min(1024, paths)
    return pl.pallas_call(
        adjoint_kernel,
        grid=(paths // tile,),
        in_specs=[
            pl.BlockSpec((stocks, tile), lambda i: (0, i)),
            pl.BlockSpec((rows, tile), lambda i: (0, i)),
            pl.BlockSpec((STEPS, rows, tile), lambda i: (0, 0, i)),
            pl.BlockSpec((1, tile), lambda i: (0, i)),
            pl.BlockSpec((STEPS, tile), lambda i: (0, i)),
            pl.BlockSpec((STEPS, tile), lambda i: (0, i)),
            pl.BlockSpec((STEPS * rows, stocks), lambda i: (0, 0)),
            pl.BlockSpec((rows, STEPS), lambda i: (0, 0)),
        ],
        out_specs=[
            pl.BlockSpec((rows, tile), lambda i: (0, i)),
            pl.BlockSpec((rows, NK), lambda i: (0, 0)),
        ],
        out_shape=[
            jax.ShapeDtypeStruct((rows, paths), jnp.float32),
            jax.ShapeDtypeStruct((rows, NK), jnp.float32),
        ],
        scratch_shapes=[pltpu.VMEM((2, STEPS * rows, stocks), jnp.bfloat16)],
        cost_estimate=pl.CostEstimate(
            flops=4 * STEPS * rows * paths * (stocks + NK),
            bytes_accessed=paths * (2 * stocks + 14 * rows),
            transcendentals=0,
        ),
        name="adjoint_surface",
    )(whole, own, shocks, value, exercise, bucket, powers, baskets)


def transition_powers(corr_gen, basket, offset, rows):
    step = time_step * corr_gen.astype(jnp.float32)
    own_step = lax.dynamic_slice_in_dim(step, offset, rows, 0)
    own_basket = lax.dynamic_slice_in_dim(basket, offset, rows, 0)
    powers = [own_step]
    for _ in range(STEPS - 1):
        powers.append(powers[-1] + own_step + jnp.dot(powers[-1], step, precision=HIGHEST))
    baskets = [own_basket]
    for power in powers[:-1]:
        baskets.append(own_basket + jnp.dot(power, basket, precision=HIGHEST))
    return jnp.concatenate(powers, axis=0), jnp.stack(baskets, axis=1)


def per_device(
    prices, loadings, basis_w, basis_bias, payoff, in_fit, cotangent, shocks, corr_gen, basket,
    exercise, bucket,
):
    stock_count = lax.axis_size("stocks")
    local_stocks, local_paths = prices.shape
    share = local_paths // stock_count
    path_count = float(local_paths * lax.axis_size("paths"))
    index = lax.axis_index("stocks")
    partial_value = lax.dot_general(
        loadings, prices, (((0,), (0,)), ((), ())), preferred_element_type=jnp.float32
    )
    factors = lax.psum_scatter(partial_value, "stocks", scatter_dimension=1, tiled=True)
    payoff_own = lax.dynamic_slice_in_dim(payoff, index * share, share, 0)
    fit_own = lax.dynamic_slice_in_dim(in_fit, index * share, share, 0)
    basis, sums = basis_and_sums(factors, basis_w, basis_bias, payoff_own, fit_own)
    sums = lax.psum(sums, ("paths", "stocks"))
    sums, cotangent = lax.optimization_barrier((sums, cotangent))
    whole = lax.all_gather(cotangent, "stocks", axis=0, tiled=True)
    coefficients = solve_coefficients(sums, path_count)
    value_own = jnp.dot(coefficients, basis.astype(jnp.float32), precision=HIGHEST)[0:1]
    value = lax.all_gather(value_own, "stocks", axis=1, tiled=True)
    powers, baskets = transition_powers(corr_gen, basket, index * local_stocks, local_stocks)
    delta_out, partial_surface = adjoint_and_surface(
        whole, cotangent, shocks, value, exercise, bucket, powers, baskets
    )
    surface = lax.psum_scatter(partial_surface, "paths", scatter_dimension=1, tiled=True)
    return (delta_out, surface)


def solution(mesh):
    return jax.shard_map(
        per_device,
        mesh=mesh,
        in_specs=(
            P("stocks", "paths"),
            P("stocks", None),
            P(),
            P(),
            P("paths"),
            P("paths"),
            P("stocks", "paths"),
            P(None, "stocks", "paths"),
            P(),
            P(),
            P(None, "paths"),
            P(None, "paths"),
        ),
        out_specs=(P("stocks", "paths"), P("stocks", "paths")),
        check_vma=False,
    )
```
